32 devices in a mesh: dp: 1 (over z), sp: 4 (over y), tp: 8 (over x, core).
Axes of the slice: x: 4, y: 4, z: 1, core: 2. Of those that a mesh axis runs over, the one named last changes fastest.
The devices are a block of a 4x4x8 slice.
Arguments:
- x: bfloat16 [4096, 3072], P(('dp', 'sp', 'tp'))
- segment_ids: int32 [4096], P(('dp', 'sp', 'tp'))
- positions: int32 [4096], P(('dp', 'sp', 'tp'))
- norm_gain: bfloat16 [4, 3072], replicated
- wq: bfloat16 [4, 3072, 3072], P(None, None, 'tp')
- wk: bfloat16 [4, 3072, 1024], P(None, None, 'tp')
- wv: bfloat16 [4, 3072, 1024], P(None, None, 'tp')
- wo: bfloat16 [4, 3072, 3072], P(None, 'tp')
- w_gate: bfloat16 [4, 3072, 8192], P(None, None, 'tp')
- w_up: bfloat16 [4, 3072, 8192], P(None, None, 'tp')
- w_down: bfloat16 [4, 8192, 3072], P(None, 'tp')
Outputs:
- output: bfloat16 [4096, 3072], P(('dp', 'sp', 'tp'))
All inputs are finite; a program needn't handle non-finite values.
Results may differ from the reference program's by a relative error of at most 0.02.
Values are sent between devices in bfloat16 or wider.
A program may use at most 768 MiB of HBM per device.

```python
import jax
import jax.numpy as jnp
from jax import lax

D = 3072
HEADS = 24
KV_HEADS = 8
HEAD = 128
FF = 8192
TOKENS = 4096
LAYERS = 4
QBLK = 64

GROUP = HEADS // KV_HEADS
ROPE_THETA = 500000.0
ATTN_GAIN = 1.2


def setup_inputs(seed: int = 0, part: int = 0) -> dict:
    key = jax.random.key(seed)
    kp = jax.random.split(jax.random.fold_in(key, part), 5)
    x = jax.random.normal(kp[0], (TOKENS, D), jnp.float32).astype(jnp.bfloat16)
    kd = jax.random.split(jax.random.fold_in(jax.random.fold_in(key, part), 7), 3)
    cuts = jnp.sort(jax.random.randint(kd[0], (5,), 1, TOKENS, dtype=jnp.int32))
    idx = jnp.arange(TOKENS, dtype=jnp.int32)
    seg = jnp.sum((idx[:, None] >= cuts[None, :]).astype(jnp.int32), axis=1).astype(jnp.int32)
    starts = jnp.concatenate([jnp.zeros((1,), jnp.int32), cuts])
    cs = jnp.cumsum(jax.random.randint(kd[1], (TOKENS,), 1, 4, dtype=jnp.int32)).astype(jnp.int32)
    off = jax.random.randint(kd[2], (6,), 0, 2048, dtype=jnp.int32)
    pos = (cs - cs[starts][seg] + off[seg]).astype(jnp.int32)
    kw = jax.random.split(jax.random.key(seed + 1), 8)
    out_gain = 2.0 * (TOKENS / 1024) ** 0.5 * (4 / LAYERS) ** 0.5
    down_gain = 0.8 * (4 / LAYERS) ** 0.5

    def draw(k, shape, scale):
        return (jax.random.normal(k, shape, jnp.float32) * scale).astype(jnp.bfloat16)

    return {
        'x': x,
        'segment_ids': seg,
        'positions': pos,
        'norm_gain': jax.random.uniform(kw[0], (LAYERS, D), jnp.float32, 0.5, 1.5).astype(jnp.bfloat16),
        'wq': draw(kw[1], (LAYERS, D, HEADS * HEAD), ATTN_GAIN * D ** -0.5),
        'wk': draw(kw[2], (LAYERS, D, KV_HEADS * HEAD), ATTN_GAIN * D ** -0.5),
        'wv': draw(kw[3], (LAYERS, D, KV_HEADS * HEAD), D ** -0.5),
        'wo': draw(kw[4], (LAYERS, HEADS * HEAD, D), out_gain * (HEADS * HEAD) ** -0.5),
        'w_gate': draw(kw[5], (LAYERS, D, FF), D ** -0.5),
        'w_up': draw(kw[6], (LAYERS, D, FF), D ** -0.5),
        'w_down': draw(kw[7], (LAYERS, FF, D), down_gain * FF ** -0.5),
    }


def rms_norm(x, g):
    xf = x.astype(jnp.float32)
    r = lax.rsqrt(jnp.mean(xf * xf, axis=-1, keepdims=True) + 1e-5)
    return (xf * r * g.astype(jnp.float32)).astype(jnp.bfloat16)


def rope(t, pos):
    half = HEAD // 2
    inv = ROPE_THETA ** (-(jnp.arange(half, dtype=jnp.float32) * (2.0 / HEAD)))
    ang = pos.astype(jnp.float32)[:, None] * inv[None, :]
    c = jnp.cos(ang)[:, None, :]
    s = jnp.sin(ang)[:, None, :]
    t1 = t[..., :half].astype(jnp.float32)
    t2 = t[..., half:].astype(jnp.float32)
    return jnp.concatenate([t1 * c - t2 * s, t2 * c + t1 * s], axis=-1).astype(jnp.bfloat16)


def attention(q, k, v, seg):
    idx = jnp.arange(TOKENS, dtype=jnp.int32)
    nb = TOKENS // QBLK
    qb = q.reshape(nb, QBLK, KV_HEADS, GROUP, HEAD)
    kf = k.astype(jnp.float32)
    vf = v.astype(jnp.float32)

    def one(args):
        qq, qi, qs = args
        sc = jnp.einsum('qkgd,skd->kgqs', qq.astype(jnp.float32), kf) * HEAD ** -0.5
        m = (idx[None, :] <= qi[:, None]) & (seg[None, :] == qs[:, None])
        sc = jnp.where(m[None, None], sc, -1e30)
        p = jax.nn.softmax(sc, axis=-1).astype(jnp.bfloat16)
        o = jnp.einsum('kgqs,skd->qkgd', p.astype(jnp.float32), vf)
        return o.astype(jnp.bfloat16)

    o = lax.map(one, (qb, idx.reshape(nb, QBLK), seg.reshape(nb, QBLK)))
    return o.reshape(TOKENS, HEADS * HEAD)


def reference(x, segment_ids, positions, norm_gain, wq, wk, wv, wo, w_gate, w_up, w_down):
    def layer(h, w):
        g, q_w, k_w, v_w, o_w, g_w, u_w, d_w = w
        n = rms_norm(h, g)
        q = jnp.dot(n, q_w, preferred_element_type=jnp.float32).astype(jnp.bfloat16).reshape(TOKENS, HEADS, HEAD)
        k = jnp.dot(n, k_w, preferred_element_type=jnp.float32).astype(jnp.bfloat16).reshape(TOKENS, KV_HEADS, HEAD)
        v = jnp.dot(n, v_w, preferred_element_type=jnp.float32).astype(jnp.bfloat16).reshape(TOKENS, KV_HEADS, HEAD)
        q = rope(q, positions)
        k = rope(k, positions)
        a = attention(q, k, v, segment_ids)
        gg = jnp.dot(n, g_w, preferred_element_type=jnp.float32).astype(jnp.bfloat16)
        uu = jnp.dot(n, u_w, preferred_element_type=jnp.float32).astype(jnp.bfloat16)
        m = (jax.nn.silu(gg.astype(jnp.float32)) * uu.astype(jnp.float32)).astype(jnp.bfloat16)
        y = (jnp.dot(a, o_w, preferred_element_type=jnp.float32) + jnp.dot(m, d_w, preferred_element_type=jnp.float32)).astype(jnp.bfloat16)
        return h + y, None

    out, _ = lax.scan(layer, x, (norm_gain, wq, wk, wv, wo, w_gate, w_up, w_down))
    return out
```

```python
import functools

import jax
import jax.numpy as jnp
from jax import lax
from jax.experimental import pallas as pl
from jax.experimental.pallas import tpu as pltpu
from jax.sharding import PartitionSpec as P

HEAD = 128
QB = 256
KB = 256
ROPE_THETA = 500000.0
EPS = 1e-5
NEG = -1e30


def rms_norm(x, g):
    xf = x.astype(jnp.float32)
    r = lax.rsqrt(jnp.mean(xf * xf, axis=-1, keepdims=True) + EPS)
    return (xf * r * g.astype(jnp.float32)).astype(jnp.bfloat16)


def rope(t, c, s):
    half = HEAD // 2
    t1 = t[..., :half].astype(jnp.float32)
    t2 = t[..., half:].astype(jnp.float32)
    return jnp.concatenate([t1 * c - t2 * s, t2 * c + t1 * s], axis=-1).astype(jnp.bfloat16)


def mm(a, b):
    return jnp.dot(a, b, preferred_element_type=jnp.float32)


def attn_kernel(grp, lo_ref, base_ref, q_ref, k_ref, v_ref, sq_ref, sk_ref, o_ref, m_s, l_s, acc_s):
    i = pl.program_id(0)
    rows = q_ref.shape[0]
    lo = lo_ref[i]
    q0 = base_ref[0] + i * rows
    hi = (q0 + rows + KB - 1) // KB
    qs = jnp.concatenate([q_ref[:, h * HEAD:(h + 1) * HEAD] for h in range(grp)], axis=0)
    m_s[...] = jnp.full(m_s.shape, NEG, jnp.float32)
    l_s[...] = jnp.zeros(l_s.shape, jnp.float32)
    acc_s[...] = jnp.zeros(acc_s.shape, jnp.float32)
    coef = HEAD ** -0.5 * 1.4426950408889634
    sq = sq_ref[...]
    qi = q0 + lax.broadcasted_iota(jnp.int32, (rows, KB), 0)

    @pl.loop(lo, hi)
    def _(j):
        k0 = pl.multiple_of(j * KB, KB)
        kb = k_ref[pl.ds(k0, KB), :]
        vb = v_ref[pl.ds(k0, KB), :]
        s = lax.dot_general(qs, kb, (((1,), (1,)), ((), ())), preferred_element_type=jnp.float32)
        ki = k0 + lax.broadcasted_iota(jnp.int32, (rows, KB), 1)
        vis = (ki <= qi) & (sk_ref[pl.ds(j, 1), :] == sq)
        s = jnp.where(vis[None], s.reshape(grp, rows, KB), NEG).reshape(grp * rows, KB)
        mp = m_s[...]
        mn = jnp.maximum(mp, jnp.max(s, axis=1, keepdims=True))
        al = jnp.exp2((mp - mn) * coef)
        p = jnp.exp2((s - mn[:, :1]) * coef)
        l_s[...] = l_s[...] * al + jnp.sum(p, axis=1, keepdims=True)
        acc_s[...] = acc_s[...] * al + mm(p.astype(jnp.bfloat16), vb)
        m_s[...] = mn

    o = (acc_s[...] / l_s[...]).astype(o_ref.dtype)
    for h in range(grp):
        o_ref[:, h * HEAD:(h + 1) * HEAD] = o[h * rows:(h + 1) * rows, :]


def attend(q, kc, vc, lo, base, sq, sk):
    tc, width = q.shape
    tall = kc.shape[0]
    grp = width // HEAD
    nb = tc // QB
    whole = lambda i, *_: (0, 0)
    rowb = lambda i, *_: (i, 0)
    return pl.pallas_call(
        functools.partial(attn_kernel, grp),
        grid_spec=pltpu.PrefetchScalarGridSpec(
            num_scalar_prefetch=2,
            grid=(nb,),
            in_specs=[
                pl.BlockSpec((QB, width), rowb),
                pl.BlockSpec((tall, HEAD), whole),
                pl.BlockSpec((tall, HEAD), whole),
                pl.BlockSpec((QB, 1), rowb),
                pl.BlockSpec((tall // KB, KB), whole),
            ],
            out_specs=pl.BlockSpec((QB, width), rowb),
            scratch_shapes=[pltpu.VMEM((grp * QB, HEAD), jnp.float32)] * 3,
        ),
        out_shape=jax.ShapeDtypeStruct((tc, width), jnp.bfloat16),
        cost_estimate=pl.CostEstimate(flops=4 * tc * width * tall // 4, bytes_accessed=4 * tc * width, transcendentals=0),
        name="attn",
    )(lo, base, q, kc, vc, sq, sk)


def solution(mesh):
    ntp = mesh.shape['tp']
    tok = P(('dp', 'sp', 'tp'))
    tok2 = P(('dp', 'sp', 'tp'), None)
    col = P(None, None, 'tp')
    row = P(None, 'tp', None)

    def body(x, seg, pos, gn, wq, wk, wv, wo, wg, wu, wd):
        tl, width = x.shape
        tc = tl * ntp
        hl = wq.shape[2] // HEAD
        s = lax.axis_index('sp')
        seg_all = lax.all_gather(seg, ('sp', 'tp'), tiled=True)
        pos_c = lax.all_gather(pos, 'tp', tiled=True)
        seg_c = lax.dynamic_slice_in_dim(seg_all, s * tc, tc)
        tall = seg_all.shape[0]
        half = HEAD // 2
        inv = ROPE_THETA ** (-(jnp.arange(half, dtype=jnp.float32) * (2.0 / HEAD)))
        ang = pos_c.astype(jnp.float32)[:, None] * inv[None, :]
        cos = jnp.cos(ang)[:, None, :]
        sin = jnp.sin(ang)[:, None, :]
        first = seg_c[::QB]
        lo = jnp.sum((seg_all[None, :] < first[:, None]).astype(jnp.int32), axis=1) // KB
        base = (s * tc).astype(jnp.int32).reshape(1)
        sq = seg_c.reshape(tc, 1)
        sk = seg_all.reshape(tall // KB, KB)
        h = x
        for j in range(gn.shape[0]):
            n = lax.all_gather(rms_norm(h, gn[j]), 'tp', tiled=True)
            k = rope(mm(n, wk[j]).astype(jnp.bfloat16), cos[:, 0], sin[:, 0])
            v = mm(n, wv[j]).astype(jnp.bfloat16)
            kv = lax.all_gather(jnp.concatenate([k, v], axis=1), 'sp', tiled=True)
            q = rope(mm(n, wq[j]).astype(jnp.bfloat16).reshape(tc, hl, HEAD), cos, sin).reshape(tc, hl * HEAD)
            gg = mm(n, wg[j]).astype(jnp.bfloat16)
            uu = mm(n, wu[j]).astype(jnp.bfloat16)
            m = (jax.nn.silu(gg.astype(jnp.float32)) * uu.astype(jnp.float32)).astype(jnp.bfloat16)
            a = attend(q, kv[:, :HEAD], kv[:, HEAD:], lo, base, sq, sk)
            part = (mm(a, wo[j]) + mm(m, wd[j])).astype(jnp.bfloat16)
            h = h + lax.psum_scatter(part, 'tp', scatter_dimension=0, tiled=True)
        return h

    return jax.shard_map(body, mesh=mesh,
                         in_specs=(tok2, tok, tok, P(), col, col, col, row, col, col, row),
                         out_specs=tok2, check_vma=False)
```

```python
import functools

import jax
import jax.numpy as jnp
from jax import lax
from jax.experimental import pallas as pl
from jax.experimental.pallas import tpu as pltpu
from jax.sharding import PartitionSpec as P

HEAD = 128
QB = 256
KB = 256
FT = 256
ROPE_THETA = 500000.0
EPS = 1e-5
NEG = -1e30
VMEM_LIMIT = 60 * 1024 * 1024
ANY = pl.BlockSpec(memory_space=pl.ANY)
VM = pl.BlockSpec(memory_space=pltpu.VMEM)


def rms_norm(x, g):
    xf = x.astype(jnp.float32)
    r = lax.rsqrt(jnp.mean(xf * xf, axis=-1, keepdims=True) + EPS)
    return (xf * r * g.astype(jnp.float32)).astype(jnp.bfloat16)


def mm(a, b):
    return jnp.dot(a, b, preferred_element_type=jnp.float32)


def attn_kernel(grp, lo_ref, base_ref, q_ref, kv_ref, sq_ref, sk_ref, o_ref, m_s, l_s, acc_s):
    i = pl.program_id(0)
    rows = q_ref.shape[0]
    lo = lo_ref[i]
    q0 = base_ref[0] + i * rows
    hi = (q0 + rows + KB - 1) // KB
    qs = jnp.concatenate([q_ref[:, h * HEAD:(h + 1) * HEAD] for h in range(grp)], axis=0)
    m_s[...] = jnp.full(m_s.shape, NEG, jnp.float32)
    l_s[...] = jnp.zeros(l_s.shape, jnp.float32)
    acc_s[...] = jnp.zeros(acc_s.shape, jnp.float32)
    coef = HEAD ** -0.5 * 1.4426950408889634
    sq = sq_ref[...]
    qi = q0 + lax.broadcasted_iota(jnp.int32, (rows, KB), 0)

    @pl.loop(lo, hi)
    def _(j):
        k0 = pl.multiple_of(j * KB, KB)
        kb = kv_ref[pl.ds(k0, KB), :HEAD]
        vb = kv_ref[pl.ds(k0, KB), HEAD:]
        s = lax.dot_general(qs, kb, (((1,), (1,)), ((), ())), preferred_element_type=jnp.float32)
        ki = k0 + lax.broadcasted_iota(jnp.int32, (rows, KB), 1)
        vis = (ki <= qi) & (sk_ref[pl.ds(j, 1), :] == sq)
        s = jnp.where(vis[None], s.reshape(grp, rows, KB), NEG).reshape(grp * rows, KB)
        mp = m_s[...]
        mn = jnp.maximum(mp, jnp.max(s, axis=1, keepdims=True))
        al = jnp.exp2((mp - mn) * coef)
        p = jnp.exp2((s - mn[:, :1]) * coef)
        l_s[...] = l_s[...] * al + jnp.sum(p, axis=1, keepdims=True)
        acc_s[...] = acc_s[...] * al + mm(p.astype(jnp.bfloat16), vb)
        m_s[...] = mn

    o = (acc_s[...] / l_s[...]).astype(o_ref.dtype)
    for h in range(grp):
        o_ref[:, h * HEAD:(h + 1) * HEAD] = o[h * rows:(h + 1) * rows, :]


def attend(q, kv, lo, base, sq, sk):
    tc, width = q.shape
    tall = kv.shape[0]
    grp = width // HEAD
    nb = tc // QB
    whole = lambda i, *_: (0, 0)
    rowb = lambda i, *_: (i, 0)
    return pl.pallas_call(
        functools.partial(attn_kernel, grp),
        grid_spec=pltpu.PrefetchScalarGridSpec(
            num_scalar_prefetch=2,
            grid=(nb,),
            in_specs=[
                pl.BlockSpec((QB, width), rowb),
                pl.BlockSpec((tall, 2 * HEAD), whole),
                pl.BlockSpec((QB, 1), rowb),
                pl.BlockSpec((tall // KB, KB), whole),
            ],
            out_specs=pl.BlockSpec((QB, width), rowb),
            scratch_shapes=[pltpu.VMEM((grp * QB, HEAD), jnp.float32)] * 3,
        ),
        out_shape=jax.ShapeDtypeStruct((tc, width), jnp.bfloat16),
        cost_estimate=pl.CostEstimate(flops=tc * width * tall, bytes_accessed=4 * tc * width, transcendentals=0),
        name="attn",
    )(lo, base, q, kv, sq, sk)


class Ring:
    def __init__(self, nx, ny, tl):
        self.nx, self.ny, self.tl, self.hf = nx, ny, tl, tl // 2
        t = lax.axis_index('tp')
        self.x = t // 2
        self.c = t % 2
        self.y = lax.axis_index('sp')
        self.right = ((self.x + 1) % nx) * 2 + self.c
        self.left = ((self.x + nx - 1) % nx) * 2 + self.c
        self.partner = self.x * 2 + 1 - self.c
        self.up = (self.y + 1) % ny
        self.down = (self.y + ny - 1) % ny

    def row(self, dx, core, h):
        return pl.multiple_of((((self.x + dx + self.nx) % self.nx) * 2 + core) * self.tl + h * self.hf, self.hf)

    def piece(self, s, i):
        side = (s * (3 - s)) // 2
        dx = side * (2 * i - 1) + 2 * (s // 3)
        flip = (s // 2) * (1 - s // 3)
        return dx, i + flip * (1 - 2 * i)


def rcopy(src, dst, ssem, rsem, dev):
    return pltpu.make_async_remote_copy(src_ref=src, dst_ref=dst, send_sem=ssem, recv_sem=rsem,
                                        device_id=dev, device_id_type=pl.DeviceIdType.MESH)


def barrier(devs):
    b = pltpu.get_barrier_semaphore()
    for d in devs:
        pl.semaphore_signal(b, inc=1, device_id=d, device_id_type=pl.DeviceIdType.MESH)
    pl.semaphore_wait(b, len(devs))


def in_kernel(l, nx, ny, n_ref, cos_ref, sin_ref, wq, wk, wv, wg, wu, q_ref, kv_ref, m_ref,
              w1, w2, w3, nb, kvs, wsem, rs, rr, ps, pr, ks, kr):
    tl = n_ref.shape[0]
    R = Ring(nx, ny, tl)
    hf, c = R.hf, R.c
    qw = wq.shape[2]
    f = wg.shape[2]
    tc = q_ref.shape[0]
    loads = [
        pltpu.make_async_copy(wq.at[l], w1.at[:, 0:qw], wsem.at[0]),
        pltpu.make_async_copy(wk.at[l], w1.at[:, qw:qw + HEAD], wsem.at[1]),
        pltpu.make_async_copy(wv.at[l], w1.at[:, qw + HEAD:qw + 2 * HEAD], wsem.at[2]),
        pltpu.make_async_copy(wg.at[l], w2, wsem.at[3]),
        pltpu.make_async_copy(wu.at[l], w3, wsem.at[4]),
    ]
    for d in loads:
        d.start()
    side = ({'tp': R.right}, {'tp': R.left})
    mate = {'tp': R.partner}
    rows_ = ({'sp': R.up}, {'sp': R.down})
    barrier([side[0], side[1], mate, rows_[0], rows_[1]])

    def slot(s, i):
        return nb.at[s, pl.ds(pl.multiple_of((2 * i + c) * hf, hf), hf), :]

    def other(s, i):
        return nb.at[s, pl.ds(pl.multiple_of((2 * i + 1 - c) * hf, hf), hf), :]

    def half(h):
        return n_ref.at[pl.ds(h * hf, hf), :]

    def ring(s, i):
        src = slot(1, i) if s == 3 else half(i if s == 1 else 1 - i)
        return rcopy(src, slot(s, i), rs.at[s, i], rr.at[s, i], side[i])

    def ring_in(s, i):
        return rcopy(slot(s, i), slot(s, i), rs.at[s, i], rr.at[s, i], side[i])

    def pass_on(s, i, src):
        return rcopy(src, slot(s, i), ps.at[s, i], pr.at[s, i], mate)

    def pass_in(s, i):
        return rcopy(other(s, i), other(s, i), ps.at[s, i], pr.at[s, i], mate)

    for i in range(2):
        ring(1, i).start()
    for i in range(2):
        pass_on(0, i, half(i)).start()
    for i in range(2):
        ring(2, i).start()
    for i in range(2):
        nb[0, pl.ds(pl.multiple_of((2 * i + c) * hf, hf), hf), :] = n_ref[i * hf:(i + 1) * hf, :]

    def kv_send(s, d):
        return rcopy(kvs.at[0, s], kvs.at[1 + d, s], ks.at[s, d], kr.at[s, d], rows_[d])

    def kv_fwd(s, d):
        part = pl.ds(d * tl, tl)
        return rcopy(kvs.at[1 + d, s, part, :], kvs.at[3, s, part, :], ks.at[s, 2 + d], kr.at[s, 2 + d], rows_[d])

    @pl.loop(0, 4)
    def _(s):
        @pl.when(s > 0)
        def _():
            for i in range(2):
                ring_in(s, i).wait_recv()
                @pl.when(s == 1)
                def _():
                    ring(3, i).start()
                pass_on(s, i, slot(s, i)).start()

        for i in range(2):
            pass_in(s, i).wait_recv()

        @pl.when(s == 0)
        def _():
            for d in loads[:3]:
                d.wait()

        offs = []
        for b in range(4):
            dx, h = R.piece(s, b // 2)
            offs.append(R.row(dx, b % 2, h))
        cs = jnp.concatenate([cos_ref[pl.ds(o, hf), :] for o in offs], axis=0)
        sn = jnp.concatenate([sin_ref[pl.ds(o, hf), :] for o in offs], axis=0)

        def rot(t):
            t = t.astype(jnp.bfloat16).astype(jnp.float32)
            return (t * cs + pltpu.roll(t, HEAD // 2, 1) * sn).astype(jnp.bfloat16)

        kv = mm(nb[s], w1[:, qw:])
        kvs[0, s, :, :HEAD] = rot(kv[:, :HEAD])
        kvs[0, s, :, HEAD:] = kv[:, HEAD:].astype(jnp.bfloat16)
        q = mm(nb[s], w1[:, :qw])
        for j in range(qw // HEAD):
            qh = rot(q[:, j * HEAD:(j + 1) * HEAD])
            for b in range(4):
                q_ref[pl.ds(offs[b], hf), j * HEAD:(j + 1) * HEAD] = qh[b * hf:(b + 1) * hf]
        for d in range(2):
            kv_send(s, d).start()

        @pl.when(s == 0)
        def _():
            for d in loads[3:]:
                d.wait()

        @pl.loop(0, f // FT)
        def _(j):
            cols = pl.ds(pl.multiple_of(j * FT, FT), FT)
            g = mm(nb[s], w2[:, cols]).astype(jnp.bfloat16).astype(jnp.float32)
            u = mm(nb[s], w3[:, cols]).astype(jnp.bfloat16).astype(jnp.float32)
            m = (g * jax.nn.sigmoid(g) * u).astype(jnp.bfloat16)
            for b in range(4):
                m_ref[pl.ds(offs[b], hf), cols] = m[b * hf:(b + 1) * hf]

        for d in range(2):
            kv_send(s, d).wait_recv()
            kv_fwd(s, d).start()

    for i in range(2):
        for s in range(1, 4):
            ring(s, i).wait_send()
        for s in range(4):
            pass_on(s, i, slot(s, i)).wait_send()

    dy = (0, ny - 1, 1, 2)

    def put(src, s):
        base = ((R.y + dy[src]) % ny) * tc
        for b in range(4):
            dx, h = R.piece(s, b // 2)
            kv_ref[pl.ds(pl.multiple_of(base + R.row(dx, b % 2, h), hf), hf), :] = kvs[src, s, b * hf:(b + 1) * hf, :]

    @pl.loop(0, 4)
    def _(s):
        for src in range(3):
            put(src, s)

    @pl.loop(0, 4)
    def _(s):
        for d in range(2):
            kv_fwd(s, d).wait_recv()
            kv_fwd(s, d).wait_send()
            kv_send(s, d).wait_send()
        put(3, s)


def stage_in(l, nx, ny, n, cosf, sinf, wq, wk, wv, wg, wu):
    tl, width = n.shape
    tc = cosf.shape[0]
    qw, f = wq.shape[2], wg.shape[2]
    bf = jnp.bfloat16
    dma = pltpu.SemaphoreType.DMA
    flops = 2 * tc * width * (qw + 2 * HEAD + 2 * f)
    return pl.pallas_call(
        functools.partial(in_kernel, l, nx, ny),
        out_shape=(jax.ShapeDtypeStruct((tc, qw), bf),
                   jax.ShapeDtypeStruct((ny * tc, 2 * HEAD), bf),
                   jax.ShapeDtypeStruct((tc, f), bf)),
        in_specs=[VM, VM, VM, ANY, ANY, ANY, ANY, ANY],
        out_specs=(VM, VM, VM),
        scratch_shapes=[
            pltpu.VMEM((width, qw + 2 * HEAD), bf),
            pltpu.VMEM((width, f), bf),
            pltpu.VMEM((width, f), bf),
            pltpu.VMEM((4, 2 * tl, width), bf),
            pltpu.VMEM((4, 4, 2 * tl, 2 * HEAD), bf),
            dma((5,)), dma((4, 2)), dma((4, 2)), dma((4, 2)), dma((4, 2)), dma((4, 4)), dma((4, 4)),
        ],
        compiler_params=pltpu.CompilerParams(collective_id=0, has_side_effects=True, vmem_limit_bytes=VMEM_LIMIT),
        cost_estimate=pl.CostEstimate(flops=flops, bytes_accessed=2 * width * (qw + 2 * HEAD + 2 * f), transcendentals=0),
        name="gather_in",
    )(n, cosf, sinf, wq, wk, wv, wg, wu)


def out_kernel(l, nx, ny, a_ref, m_ref, h_ref, g_ref, wo, wd, ho_ref, no_ref,
               w1, w2, own, psend, precv, csend, rin, wsem, ps, pr, rs, rr):
    tl, width = h_ref.shape
    R = Ring(nx, ny, tl)
    hf, c = R.hf, R.c
    nt = min(512, width)
    loads = [pltpu.make_async_copy(wo.at[l], w1, wsem.at[0]), pltpu.make_async_copy(wd.at[l], w2, wsem.at[1])]
    for d in loads:
        d.start()
    side = ({'tp': R.right}, {'tp': R.left})
    mate = {'tp': R.partner}
    barrier([side[0], side[1], mate])
    for d in loads:
        d.wait()

    dest = (((2, 0), (2, 1)), ((1, 1), (-1, 0)), ((1, 0), (-1, 1)), ((0, 0), (0, 1)))

    def give(s):
        return rcopy(psend.at[s], precv.at[s], ps.at[s], pr.at[s], mate)

    def send(s, i):
        part = pl.ds(i * hf, hf)
        return rcopy(csend.at[s, part, :], rin.at[s, part, :], rs.at[s, i], rr.at[s, i], side[i])

    def compute(s):
        offs = [R.row(dx, core, h) for core in (1 - c, c) for dx, h in dest[s]]

        @pl.loop(0, width // nt)
        def _(j):
            cols = pl.ds(pl.multiple_of(j * nt, nt), nt)
            la = jnp.concatenate([a_ref[pl.ds(o, hf), :] for o in offs], axis=0)
            lm = jnp.concatenate([m_ref[pl.ds(o, hf), :] for o in offs], axis=0)
            y = mm(la, w1[:, cols]) + mm(lm, w2[:, cols])
            psend[s, :, cols] = y[:tl].astype(jnp.bfloat16)
            own[:, cols] = y[tl:]

        give(s).start()

    def combine(s):
        give(s).wait_recv()

        @pl.loop(0, width // nt)
        def _(j):
            cols = pl.ds(pl.multiple_of(j * nt, nt), nt)
            t = own[:, cols] + precv[s, :, cols].astype(jnp.float32)
            if s == 2:
                t = t + rin[0, :, cols].astype(jnp.float32)
            csend[s, :, cols] = t.astype(jnp.bfloat16)

        for i in range(2):
            send(s, i).start()

    for s in range(3):
        compute(s)
        if s == 2:
            for i in range(2):
                send(0, i).wait_recv()
        combine(s)
    compute(3)
    give(3).wait_recv()
    for s in (1, 2):
        for i in range(2):
            send(s, i).wait_recv()

    rb = 16

    @pl.loop(0, tl // rb)
    def _(r):
        rows = pl.ds(pl.multiple_of(r * rb, rb), rb)
        top = r // (hf // rb)
        sl = 2 - top
        sr = 1 + top
        inner = pl.multiple_of((r % (hf // rb)) * rb, rb)
        lrow = pl.ds(inner, rb)
        rrow = pl.ds(pl.multiple_of(hf + inner, rb), rb)
        y = own[rows, :] + precv[3, rows, :].astype(jnp.float32)
        y = y + rin[sl, lrow, :].astype(jnp.float32) + rin[sr, rrow, :].astype(jnp.float32)
        hn = (h_ref[rows, :].astype(jnp.float32) + y.astype(jnp.bfloat16).astype(jnp.float32)).astype(jnp.bfloat16)
        ho_ref[rows, :] = hn
        hf32 = hn.astype(jnp.float32)
        inv = lax.rsqrt(jnp.mean(hf32 * hf32, axis=1, keepdims=True) + EPS)
        no_ref[rows, :] = (hf32 * inv * g_ref[...].astype(jnp.float32)).astype(jnp.bfloat16)

    for s in range(4):
        give(s).wait_send()
    for s in range(3):
        for i in range(2):
            send(s, i).wait_send()


def stage_out(l, nx, ny, a, m, h, g, wo, wd):
    tl, width = h.shape
    tc, qw = a.shape
    f = m.shape[1]
    bf = jnp.bfloat16
    dma = pltpu.SemaphoreType.DMA
    return pl.pallas_call(
        functools.partial(out_kernel, l, nx, ny),
        out_shape=(jax.ShapeDtypeStruct((tl, width), bf), jax.ShapeDtypeStruct((tl, width), bf)),
        in_specs=[VM, VM, VM, VM, ANY, ANY],
        out_specs=(VM, VM),
        scratch_shapes=[
            pltpu.VMEM((qw, width), bf),
            pltpu.VMEM((f, width), bf),
            pltpu.VMEM((tl, width), jnp.float32),
            pltpu.VMEM((4, tl, width), bf),
            pltpu.VMEM((4, tl, width), bf),
            pltpu.VMEM((3, tl, width), bf),
            pltpu.VMEM((3, tl, width), bf),
            dma((2,)), dma((4,)), dma((4,)), dma((3, 2)), dma((3, 2)),
        ],
        compiler_params=pltpu.CompilerParams(collective_id=1, has_side_effects=True, vmem_limit_bytes=VMEM_LIMIT),
        cost_estimate=pl.CostEstimate(flops=2 * tc * width * (qw + f), bytes_accessed=2 * width * (qw + f), transcendentals=0),
        name="out_scatter",
    )(a, m, h, g, wo, wd)


def solution(mesh):
    nsp = mesh.shape['sp']
    ntp = mesh.shape['tp']
    assert ntp == 8 and nsp == 4
    tok = P(('dp', 'sp', 'tp'))
    tok2 = P(('dp', 'sp', 'tp'), None)
    col = P(None, None, 'tp')
    row = P(None, 'tp', None)

    def body(x, seg, pos, gn, wq, wk, wv, wo, wg, wu, wd):
        tl = x.shape[0]
        tc = tl * ntp
        s = lax.axis_index('sp')
        seg_all = lax.all_gather(seg, ('sp', 'tp'), tiled=True)
        pos_c = lax.all_gather(pos, 'tp', tiled=True)
        seg_c = lax.dynamic_slice_in_dim(seg_all, s * tc, tc)
        tall = seg_all.shape[0]
        half = HEAD // 2
        inv = ROPE_THETA ** (-(jnp.arange(half, dtype=jnp.float32) * (2.0 / HEAD)))
        ang = pos_c.astype(jnp.float32)[:, None] * inv[None, :]
        cos, sin = jnp.cos(ang), jnp.sin(ang)
        cosf = jnp.concatenate([cos, cos], axis=1)
        sinf = jnp.concatenate([-sin, sin], axis=1)
        first = seg_c[::QB]
        lo = jnp.sum((seg_all[None, :] < first[:, None]).astype(jnp.int32), axis=1) // KB
        base = (s * tc).astype(jnp.int32).reshape(1)
        sq = seg_c.reshape(tc, 1)
        sk = seg_all.reshape(tall // KB, KB)
        h = x
        n = rms_norm(h, gn[0])
        nl = gn.shape[0]
        for j in range(nl):
            q, kv, m = stage_in(j, ntp // 2, nsp, n, cosf, sinf, wq, wk, wv, wg, wu)
            a = attend(q, kv, lo, base, sq, sk)
            g = gn[min(j + 1, nl - 1)].reshape(1, -1)
            h, n = stage_out(j, ntp // 2, nsp, a, m, h, g, wo, wd)
        return h

    return jax.shard_map(body, mesh=mesh,
                         in_specs=(tok2, tok, tok, P(), col, col, col, row, col, col, row),
                         out_specs=tok2, check_vma=False)
```

```python
import functools

import jax
import jax.numpy as jnp
from jax import lax
from jax.experimental import pallas as pl
from jax.experimental.pallas import tpu as pltpu
from jax.sharding import PartitionSpec as P

HEAD = 128
QB = 256
KB = 256
FT = 256
ROPE_THETA = 500000.0
EPS = 1e-5
NEG = -1e30
VMEM_LIMIT = 60 * 1024 * 1024
ANY = pl.BlockSpec(memory_space=pl.ANY)
VM = pl.BlockSpec(memory_space=pltpu.VMEM)


def rms_norm(x, g):
    xf = x.astype(jnp.float32)
    r = lax.rsqrt(jnp.mean(xf * xf, axis=-1, keepdims=True) + EPS)
    return (xf * r * g.astype(jnp.float32)).astype(jnp.bfloat16)


def mm(a, b):
    return jnp.dot(a, b, preferred_element_type=jnp.float32)


def attn_kernel(grp, lo_ref, base_ref, q_ref, kv_ref, st_ref, o_ref, m_s, l_s, acc_s):
    i = pl.program_id(0)
    rows = q_ref.shape[0]
    lo = lo_ref[i]
    q0 = base_ref[0] + i * rows
    hi = (q0 + rows + KB - 1) // KB
    qs = jnp.concatenate([q_ref[:, h * HEAD:(h + 1) * HEAD] for h in range(grp)], axis=0)
    m_s[...] = jnp.full(m_s.shape, NEG, jnp.float32)
    l_s[...] = jnp.zeros(l_s.shape, jnp.float32)
    acc_s[...] = jnp.zeros(acc_s.shape, jnp.float32)
    coef = HEAD ** -0.5 * 1.4426950408889634
    st = st_ref[0]
    qi = q0 + lax.broadcasted_iota(jnp.int32, (1, rows), 1)
    kr = lax.broadcasted_iota(jnp.int32, (KB, rows), 0)

    @pl.loop(lo, hi)
    def _(j):
        k0 = pl.multiple_of(j * KB, KB)
        kb = kv_ref[pl.ds(k0, KB), :HEAD]
        vb = kv_ref[pl.ds(k0, KB), HEAD:]
        s = lax.dot_general(kb, qs, (((1,), (1,)), ((), ())), preferred_element_type=jnp.float32)
        vis = (kr >= st - k0) & (kr <= qi - k0)
        for h in range(grp):
            c = slice(h * rows, (h + 1) * rows)
            sh = jnp.where(vis, s[:, c], NEG)
            mp = m_s[:, c]
            mn = jnp.maximum(mp, jnp.max(sh, axis=0, keepdims=True))
            al = jnp.exp2((mp - mn) * coef)
            p = jnp.exp2((sh - mn) * coef)
            l_s[:, c] = l_s[:, c] * al + jnp.sum(p, axis=0, keepdims=True)
            pv = lax.dot_general(vb, p.astype(jnp.bfloat16), (((0,), (0,)), ((), ())),
                                 preferred_element_type=jnp.float32)
            acc_s[:, c] = acc_s[:, c] * al + pv
            m_s[:, c] = mn

    for h in range(grp):
        c = slice(h * rows, (h + 1) * rows)
        o_ref[:, h * HEAD:(h + 1) * HEAD] = (acc_s[:, c] / l_s[:, c]).T.astype(o_ref.dtype)


def attend(q, kv, lo, base, st):
    tc, width = q.shape
    tall = kv.shape[0]
    grp = width // HEAD
    nb = tc // QB
    whole = lambda i, *_: (0, 0)
    rowb = lambda i, *_: (i, 0)
    return pl.pallas_call(
        functools.partial(attn_kernel, grp),
        grid_spec=pltpu.PrefetchScalarGridSpec(
            num_scalar_prefetch=2,
            grid=(nb,),
            in_specs=[
                pl.BlockSpec((QB, width), rowb),
                pl.BlockSpec((tall, 2 * HEAD), whole),
                pl.BlockSpec((1, 1, QB), lambda i, *_: (i, 0, 0)),
            ],
            out_specs=pl.BlockSpec((QB, width), rowb),
            scratch_shapes=[pltpu.VMEM((1, grp * QB), jnp.float32), pltpu.VMEM((1, grp * QB), jnp.float32),
                            pltpu.VMEM((HEAD, grp * QB), jnp.float32)],
        ),
        out_shape=jax.ShapeDtypeStruct((tc, width), jnp.bfloat16),
        cost_estimate=pl.CostEstimate(flops=tc * width * tall, bytes_accessed=4 * tc * width, transcendentals=0),
        name="attn",
    )(lo, base, q, kv, st)


class Ring:
    def __init__(self, nx, ny, tl):
        self.nx, self.ny, self.tl, self.hf = nx, ny, tl, tl // 2
        t = lax.axis_index('tp')
        self.x = t // 2
        self.c = t % 2
        self.y = lax.axis_index('sp')
        self.right = ((self.x + 1) % nx) * 2 + self.c
        self.left = ((self.x + nx - 1) % nx) * 2 + self.c
        self.partner = self.x * 2 + 1 - self.c
        self.up = (self.y + 1) % ny
        self.down = (self.y + ny - 1) % ny

    def row(self, dx, core, h):
        return pl.multiple_of((((self.x + dx + self.nx) % self.nx) * 2 + core) * self.tl + h * self.hf, self.hf)

    def piece(self, s, i):
        side = (s * (3 - s)) // 2
        dx = side * (2 * i - 1) + 2 * (s // 3)
        flip = (s // 2) * (1 - s // 3)
        return dx, i + flip * (1 - 2 * i)


def rcopy(src, dst, ssem, rsem, dev):
    return pltpu.make_async_remote_copy(src_ref=src, dst_ref=dst, send_sem=ssem, recv_sem=rsem,
                                        device_id=dev, device_id_type=pl.DeviceIdType.MESH)


def barrier(devs):
    b = pltpu.get_barrier_semaphore()
    for d in devs:
        pl.semaphore_signal(b, inc=1, device_id=d, device_id_type=pl.DeviceIdType.MESH)
    pl.semaphore_wait(b, len(devs))


def ids_kernel(nsp, ntp, i_ref, o_ref, ss, rr, s2, r2):
    y, t = lax.axis_index('sp'), lax.axis_index('tp')
    peers = [{'tp': (t + d) % ntp} for d in range(1, ntp)]
    rows = [{'sp': (y + d) % nsp} for d in range(1, nsp)]
    barrier(peers + rows)
    first = [rcopy(i_ref, o_ref.at[y, t], ss.at[d], rr.at[d], peers[d]) for d in range(ntp - 1)]
    for d in first:
        d.start()
    o_ref[y, t] = i_ref[...]
    for d in range(ntp - 1):
        src = (t + ntp - d - 1) % ntp
        rcopy(o_ref.at[y, src], o_ref.at[y, src], ss.at[d], rr.at[d], peers[d]).wait_recv()
    second = [rcopy(o_ref.at[y], o_ref.at[y], s2.at[d], r2.at[d], rows[d]) for d in range(nsp - 1)]
    for d in second:
        d.start()
    for d in range(nsp - 1):
        src = (y + nsp - d - 1) % nsp
        rcopy(o_ref.at[src], o_ref.at[src], s2.at[d], r2.at[d], rows[d]).wait_recv()
    for d in first + second:
        d.wait_send()


def gather_ids(nsp, ntp, seg, pos):
    tl = seg.shape[0]
    own = jnp.zeros((8, tl), jnp.int32).at[0].set(seg).at[1].set(pos)
    dma = pltpu.SemaphoreType.DMA
    return pl.pallas_call(
        functools.partial(ids_kernel, nsp, ntp),
        out_shape=jax.ShapeDtypeStruct((nsp, ntp, 8, tl), jnp.int32),
        in_specs=[VM],
        out_specs=VM,
        scratch_shapes=[dma((ntp - 1,)), dma((ntp - 1,)), dma((nsp - 1,)), dma((nsp - 1,))],
        compiler_params=pltpu.CompilerParams(collective_id=2, has_side_effects=True),
        name="ids",
    )(own)


def in_kernel(l, nx, ny, n_ref, cos_hbm, sin_hbm, wq, wk, wv, wg, wu, q_ref, kv_ref, m_out,
              cos_ref, sin_ref, m_ref, osem, w1, w2, w3, nb, kvs, wsem, rs, rr, ps, pr, ks, kr):
    tl = n_ref.shape[0]
    R = Ring(nx, ny, tl)
    hf, c = R.hf, R.c
    qw = wq.shape[2]
    f = wg.shape[2]
    tc = q_ref.shape[0]
    loads = [
        pltpu.make_async_copy(wq.at[l], w1.at[:, 0:qw], wsem.at[0]),
        pltpu.make_async_copy(wk.at[l], w1.at[:, qw:qw + HEAD], wsem.at[1]),
        pltpu.make_async_copy(wv.at[l], w1.at[:, qw + HEAD:qw + 2 * HEAD], wsem.at[2]),
        pltpu.make_async_copy(cos_hbm, cos_ref, wsem.at[5]),
        pltpu.make_async_copy(sin_hbm, sin_ref, wsem.at[6]),
        pltpu.make_async_copy(wg.at[l], w2, wsem.at[3]),
        pltpu.make_async_copy(wu.at[l], w3, wsem.at[4]),
    ]
    for d in loads:
        d.start()
    side = ({'tp': R.right}, {'tp': R.left})
    mate = {'tp': R.partner}
    rows_ = ({'sp': R.up}, {'sp': R.down})
    barrier([side[0], side[1], mate, rows_[0], rows_[1]])

    def slot(s, i):
        return nb.at[s, pl.ds(pl.multiple_of((2 * i + c) * hf, hf), hf), :]

    def other(s, i):
        return nb.at[s, pl.ds(pl.multiple_of((2 * i + 1 - c) * hf, hf), hf), :]

    def half(h):
        return n_ref.at[pl.ds(h * hf, hf), :]

    def ring(s, i):
        src = slot(1, i) if s == 3 else half(i if s == 1 else 1 - i)
        return rcopy(src, slot(s, i), rs.at[s, i], rr.at[s, i], side[i])

    def ring_in(s, i):
        return rcopy(slot(s, i), slot(s, i), rs.at[s, i], rr.at[s, i], side[i])

    def pass_on(s, i, src):
        return rcopy(src, slot(s, i), ps.at[s, i], pr.at[s, i], mate)

    def pass_in(s, i):
        return rcopy(other(s, i), other(s, i), ps.at[s, i], pr.at[s, i], mate)

    for i in range(2):
        ring(1, i).start()
    for i in range(2):
        pass_on(0, i, half(i)).start()
    for i in range(2):
        ring(2, i).start()
    for i in range(2):
        nb[0, pl.ds(pl.multiple_of((2 * i + c) * hf, hf), hf), :] = n_ref[i * hf:(i + 1) * hf, :]

    def kv_send(s, d):
        return rcopy(kvs.at[0, s], kvs.at[1 + d, s], ks.at[s, d], kr.at[s, d], rows_[d])

    def kv_fwd(s, d):
        part = pl.ds(d * tl, tl)
        return rcopy(kvs.at[1 + d, s, part, :], kvs.at[3, s, part, :], ks.at[s, 2 + d], kr.at[s, 2 + d], rows_[d])

    def m_copy(s, b, o):
        return pltpu.make_async_copy(m_ref.at[pl.ds(o, hf), :], m_out.at[pl.ds(o, hf), :], osem.at[s, b])

    @pl.loop(0, 4)
    def _(s):
        @pl.when(s > 0)
        def _():
            for i in range(2):
                ring_in(s, i).wait_recv()
                @pl.when(s == 1)
                def _():
                    ring(3, i).start()
                pass_on(s, i, slot(s, i)).start()

        for i in range(2):
            pass_in(s, i).wait_recv()

        @pl.when(s == 0)
        def _():
            for d in loads[:5]:
                d.wait()

        offs = []
        for b in range(4):
            dx, h = R.piece(s, b // 2)
            offs.append(R.row(dx, b % 2, h))
        cs = jnp.concatenate([cos_ref[pl.ds(o, hf), :] for o in offs], axis=0)
        sn = jnp.concatenate([sin_ref[pl.ds(o, hf), :] for o in offs], axis=0)

        def rot(t):
            t = t.astype(jnp.bfloat16).astype(jnp.float32)
            return (t * cs + pltpu.roll(t, HEAD // 2, 1) * sn).astype(jnp.bfloat16)

        kv = mm(nb[s], w1[:, qw:])
        kvs[0, s, :, :HEAD] = rot(kv[:, :HEAD])
        kvs[0, s, :, HEAD:] = kv[:, HEAD:].astype(jnp.bfloat16)
        q = mm(nb[s], w1[:, :qw])
        for j in range(qw // HEAD):
            qh = rot(q[:, j * HEAD:(j + 1) * HEAD])
            for b in range(4):
                q_ref[pl.ds(offs[b], hf), j * HEAD:(j + 1) * HEAD] = qh[b * hf:(b + 1) * hf]
        for d in range(2):
            kv_send(s, d).start()

        @pl.when(s == 0)
        def _():
            for d in loads[5:]:
                d.wait()

        @pl.loop(0, f // FT)
        def _(j):
            cols = pl.ds(pl.multiple_of(j * FT, FT), FT)
            g = mm(nb[s], w2[:, cols]).astype(jnp.bfloat16).astype(jnp.float32)
            u = mm(nb[s], w3[:, cols]).astype(jnp.bfloat16).astype(jnp.float32)
            m = (g * jax.nn.sigmoid(g) * u).astype(jnp.bfloat16)
            for b in range(4):
                m_ref[pl.ds(offs[b], hf), cols] = m[b * hf:(b + 1) * hf]

        for d in range(2):
            kv_send(s, d).wait_recv()
            kv_fwd(s, d).start()
        for b in range(4):
            m_copy(s, b, offs[b]).start()

    for i in range(2):
        for s in range(1, 4):
            ring(s, i).wait_send()
        for s in range(4):
            pass_on(s, i, slot(s, i)).wait_send()

    dy = (0, ny - 1, 1, 2)

    def put(src, s):
        base = ((R.y + dy[src]) % ny) * tc
        for b in range(4):
            dx, h = R.piece(s, b // 2)
            kv_ref[pl.ds(pl.multiple_of(base + R.row(dx, b % 2, h), hf), hf), :] = kvs[src, s, b * hf:(b + 1) * hf, :]

    @pl.loop(0, 4)
    def _(s):
        for src in range(3):
            put(src, s)

    @pl.loop(0, 4)
    def _(s):
        for d in range(2):
            kv_fwd(s, d).wait_recv()
            kv_fwd(s, d).wait_send()
            kv_send(s, d).wait_send()
        for b in range(4):
            m_copy(s, b, b * hf).wait()
        put(3, s)


def stage_in(l, nx, ny, n, cosf, sinf, wq, wk, wv, wg, wu):
    tl, width = n.shape
    tc = cosf.shape[0]
    qw, f = wq.shape[2], wg.shape[2]
    bf = jnp.bfloat16
    dma = pltpu.SemaphoreType.DMA
    flops = 2 * tc * width * (qw + 2 * HEAD + 2 * f)
    return pl.pallas_call(
        functools.partial(in_kernel, l, nx, ny),
        out_shape=(jax.ShapeDtypeStruct((tc, qw), bf),
                   jax.ShapeDtypeStruct((ny * tc, 2 * HEAD), bf),
                   jax.ShapeDtypeStruct((tc, f), bf)),
        in_specs=[VM, ANY, ANY, ANY, ANY, ANY, ANY, ANY],
        out_specs=(VM, VM, ANY),
        scratch_shapes=[
            pltpu.VMEM((tc, HEAD), jnp.float32),
            pltpu.VMEM((tc, HEAD), jnp.float32),
            pltpu.VMEM((tc, f), bf),
            dma((4, 4)),
            pltpu.VMEM((width, qw + 2 * HEAD), bf),
            pltpu.VMEM((width, f), bf),
            pltpu.VMEM((width, f), bf),
            pltpu.VMEM((4, 2 * tl, width), bf),
            pltpu.VMEM((4, 4, 2 * tl, 2 * HEAD), bf),
            dma((7,)), dma((4, 2)), dma((4, 2)), dma((4, 2)), dma((4, 2)), dma((4, 4)), dma((4, 4)),
        ],
        compiler_params=pltpu.CompilerParams(collective_id=0, has_side_effects=True, vmem_limit_bytes=VMEM_LIMIT),
        cost_estimate=pl.CostEstimate(flops=flops, bytes_accessed=2 * width * (qw + 2 * HEAD + 2 * f), transcendentals=0),
        name="gather_in",
    )(n, cosf, sinf, wq, wk, wv, wg, wu)


def out_kernel(l, nx, ny, a_ref, m_ref, h_ref, g_ref, wo, wd, ho_ref, no_ref,
               w1, w2, own, psend, precv, csend, rin, wsem, ps, pr, rs, rr):
    tl, width = h_ref.shape
    R = Ring(nx, ny, tl)
    hf, c = R.hf, R.c
    nt = min(512, width)

    def load(j):
        cols = pl.ds(pl.multiple_of(j * nt, nt), nt)
        return (pltpu.make_async_copy(wo.at[l, :, cols], w1.at[:, cols], wsem.at[j, 0]),
                pltpu.make_async_copy(wd.at[l, :, cols], w2.at[:, cols], wsem.at[j, 1]))

    for j in range(width // nt):
        for d in load(j):
            d.start()
    side = ({'tp': R.right}, {'tp': R.left})
    mate = {'tp': R.partner}
    barrier([side[0], side[1], mate])

    dest = (((2, 0), (2, 1)), ((1, 1), (-1, 0)), ((1, 0), (-1, 1)), ((0, 0), (0, 1)))

    def give(s):
        return rcopy(psend.at[s], precv.at[s], ps.at[s], pr.at[s], mate)

    def send(s, i):
        part = pl.ds(i * hf, hf)
        return rcopy(csend.at[s, part, :], rin.at[s, part, :], rs.at[s, i], rr.at[s, i], side[i])

    def compute(s):
        offs = [R.row(dx, core, h) for core in (1 - c, c) for dx, h in dest[s]]

        @pl.loop(0, width // nt)
        def _(j):
            if s == 0:
                for d in load(j):
                    d.wait()
            cols = pl.ds(pl.multiple_of(j * nt, nt), nt)
            la = jnp.concatenate([a_ref[pl.ds(o, hf), :] for o in offs], axis=0)
            lm = jnp.concatenate([m_ref[pl.ds(o, hf), :] for o in offs], axis=0)
            y = mm(la, w1[:, cols]) + mm(lm, w2[:, cols])
            psend[s, :, cols] = y[:tl].astype(jnp.bfloat16)
            own[:, cols] = y[tl:]

        give(s).start()

    def combine(s):
        give(s).wait_recv()

        @pl.loop(0, width // nt)
        def _(j):
            cols = pl.ds(pl.multiple_of(j * nt, nt), nt)
            t = own[:, cols] + precv[s, :, cols].astype(jnp.float32)
            if s == 2:
                t = t + rin[0, :, cols].astype(jnp.float32)
            csend[s, :, cols] = t.astype(jnp.bfloat16)

        for i in range(2):
            send(s, i).start()

    for s in range(3):
        compute(s)
        if s == 2:
            for i in range(2):
                send(0, i).wait_recv()
        combine(s)
    compute(3)
    give(3).wait_recv()
    for s in (1, 2):
        for i in range(2):
            send(s, i).wait_recv()

    rb = 16

    @pl.loop(0, tl // rb)
    def _(r):
        rows = pl.ds(pl.multiple_of(r * rb, rb), rb)
        top = r // (hf // rb)
        sl = 2 - top
        sr = 1 + top
        inner = pl.multiple_of((r % (hf // rb)) * rb, rb)
        lrow = pl.ds(inner, rb)
        rrow = pl.ds(pl.multiple_of(hf + inner, rb), rb)
        y = own[rows, :] + precv[3, rows, :].astype(jnp.float32)
        y = y + rin[sl, lrow, :].astype(jnp.float32) + rin[sr, rrow, :].astype(jnp.float32)
        hn = (h_ref[rows, :].astype(jnp.float32) + y.astype(jnp.bfloat16).astype(jnp.float32)).astype(jnp.bfloat16)
        ho_ref[rows, :] = hn
        hf32 = hn.astype(jnp.float32)
        inv = lax.rsqrt(jnp.mean(hf32 * hf32, axis=1, keepdims=True) + EPS)
        no_ref[rows, :] = (hf32 * inv * g_ref[...].astype(jnp.float32)).astype(jnp.bfloat16)

    for s in range(4):
        give(s).wait_send()
    for s in range(3):
        for i in range(2):
            send(s, i).wait_send()


def stage_out(l, nx, ny, a, m, h, g, wo, wd):
    tl, width = h.shape
    tc, qw = a.shape
    f = m.shape[1]
    bf = jnp.bfloat16
    dma = pltpu.SemaphoreType.DMA
    return pl.pallas_call(
        functools.partial(out_kernel, l, nx, ny),
        out_shape=(jax.ShapeDtypeStruct((tl, width), bf), jax.ShapeDtypeStruct((tl, width), bf)),
        in_specs=[VM, VM, VM, VM, ANY, ANY],
        out_specs=(VM, VM),
        scratch_shapes=[
            pltpu.VMEM((qw, width), bf),
            pltpu.VMEM((f, width), bf),
            pltpu.VMEM((tl, width), jnp.float32),
            pltpu.VMEM((4, tl, width), bf),
            pltpu.VMEM((4, tl, width), bf),
            pltpu.VMEM((3, tl, width), bf),
            pltpu.VMEM((3, tl, width), bf),
            dma((width // min(512, width), 2)), dma((4,)), dma((4,)), dma((3, 2)), dma((3, 2)),
        ],
        compiler_params=pltpu.CompilerParams(collective_id=1, has_side_effects=True, vmem_limit_bytes=VMEM_LIMIT),
        cost_estimate=pl.CostEstimate(flops=2 * tc * width * (qw + f), bytes_accessed=2 * width * (qw + f), transcendentals=0),
        name="out_scatter",
    )(a, m, h, g, wo, wd)


def solution(mesh):
    nsp = mesh.shape['sp']
    ntp = mesh.shape['tp']
    assert ntp == 8 and nsp == 4
    tok = P(('dp', 'sp', 'tp'))
    tok2 = P(('dp', 'sp', 'tp'), None)
    col = P(None, None, 'tp')
    row = P(None, 'tp', None)

    def body(x, seg, pos, gn, wq, wk, wv, wo, wg, wu, wd):
        tl = x.shape[0]
        tc = tl * ntp
        s = lax.axis_index('sp')
        ids = gather_ids(nsp, ntp, seg, pos)
        seg_all = ids[:, :, 0, :].reshape(nsp * tc)
        mine = lax.dynamic_index_in_dim(ids, s, 0, keepdims=False)
        seg_c = mine[:, 0, :].reshape(tc)
        pos_c = mine[:, 1, :].reshape(tc)
        half = HEAD // 2
        inv = ROPE_THETA ** (-(jnp.arange(half, dtype=jnp.float32) * (2.0 / HEAD)))
        ang = pos_c.astype(jnp.float32)[:, None] * inv[None, :]
        cos, sin = jnp.cos(ang), jnp.sin(ang)
        cosf = jnp.concatenate([cos, cos], axis=1)
        sinf = jnp.concatenate([-sin, sin], axis=1)
        st = jnp.sum((seg_all[:, None] < seg_c[None, :]).astype(jnp.int32), axis=0)
        lo = st[::QB] // KB
        base = (s * tc).astype(jnp.int32).reshape(1)
        st = st.reshape(tc // QB, 1, QB)
        h = x
        n = rms_norm(h, gn[0])
        nl = gn.shape[0]
        for j in range(nl):
            q, kv, m = stage_in(j, ntp // 2, nsp, n, cosf, sinf, wq, wk, wv, wg, wu)
            a = attend(q, kv, lo, base, st)
            g = gn[min(j + 1, nl - 1)].reshape(1, -1)
            h, n = stage_out(j, ntp // 2, nsp, a, m, h, g, wo, wd)
        return h

    return jax.shard_map(body, mesh=mesh,
                         in_specs=(tok2, tok, tok, P(), col, col, col, row, col, col, row),
                         out_specs=tok2, check_vma=False)
```

```python
import functools

import jax
import jax.numpy as jnp
from jax import lax
from jax.experimental import pallas as pl
from jax.experimental.pallas import tpu as pltpu
from jax.sharding import PartitionSpec as P

HEAD = 128
QB = 256
KB = 256
FT = 256
RC = 64
ROPE_THETA = 500000.0
EPS = 1e-5
NEG = -1e30
VMEM_LIMIT = 60 * 1024 * 1024
ANY = pl.BlockSpec(memory_space=pl.ANY)
VM = pl.BlockSpec(memory_space=pltpu.VMEM)


def rms_norm(x, g):
    xf = x.astype(jnp.float32)
    r = lax.rsqrt(jnp.mean(xf * xf, axis=-1, keepdims=True) + EPS)
    return (xf * r * g.astype(jnp.float32)).astype(jnp.bfloat16)


def mm(a, b):
    return jnp.dot(a, b, preferred_element_type=jnp.float32)


def attn_kernel(grp, lo_ref, base_ref, q_ref, kv_ref, st_ref, o_ref, m_s, l_s, acc_s, s_s, p_s):
    i = pl.program_id(0)
    rows = q_ref.shape[0]
    lo = lo_ref[i]
    q0 = base_ref[0] + i * rows
    hi = (q0 + rows + KB - 1) // KB
    qs = jnp.concatenate([q_ref[:, h * HEAD:(h + 1) * HEAD] for h in range(grp)], axis=0)
    m_s[...] = jnp.full(m_s.shape, NEG, jnp.float32)
    l_s[...] = jnp.zeros(l_s.shape, jnp.float32)
    acc_s[...] = jnp.zeros(acc_s.shape, jnp.float32)
    coef = HEAD ** -0.5 * 1.4426950408889634
    st = st_ref[0]
    qi = q0 + lax.broadcasted_iota(jnp.int32, (1, rows), 1)
    kr = lax.broadcasted_iota(jnp.int32, (RC, rows), 0)
    heads = [slice(h * rows, (h + 1) * rows) for h in range(grp)]
    parts = [slice(r * RC, (r + 1) * RC) for r in range(KB // RC)]
    fold = lambda t: t.reshape(RC // 8, 8, rows)

    @pl.loop(lo, hi)
    def _(j):
        k0 = pl.multiple_of(j * KB, KB)
        kb = kv_ref[pl.ds(k0, KB), :HEAD]
        vb = kv_ref[pl.ds(k0, KB), HEAD:]
        for c in heads:
            s_s[:, c] = lax.dot_general(kb, qs[c], (((1,), (1,)), ((), ())), preferred_element_type=jnp.float32)
        top = [jnp.full((8, rows), NEG, jnp.float32)] * grp
        for r in range(KB // RC):
            ka = kr + (k0 + r * RC)
            vis = (ka >= st) & (ka <= qi)
            for h, c in enumerate(heads):
                t = jnp.where(vis, s_s[parts[r], c], NEG)
                s_s[parts[r], c] = t
                top[h] = jnp.maximum(top[h], jnp.max(fold(t), axis=0))
        for h, c in enumerate(heads):
            mp = m_s[:, c]
            mn = jnp.maximum(mp, jnp.max(top[h], axis=0, keepdims=True))
            al = jnp.exp2((mp - mn) * coef)
            tot = jnp.zeros((8, rows), jnp.float32)
            for r in range(KB // RC):
                p = jnp.exp2((s_s[parts[r], c] - mn) * coef)
                tot = tot + jnp.sum(fold(p), axis=0)
                p_s[parts[r], c] = p.astype(jnp.bfloat16)
            l_s[:, c] = l_s[:, c] * al + jnp.sum(tot, axis=0, keepdims=True)
            pv = lax.dot_general(vb, p_s[:, c], (((0,), (0,)), ((), ())), preferred_element_type=jnp.float32)
            acc_s[:, c] = acc_s[:, c] * al + pv
            m_s[:, c] = mn

    for h in range(grp):
        c = slice(h * rows, (h + 1) * rows)
        o_ref[:, h * HEAD:(h + 1) * HEAD] = (acc_s[:, c] / l_s[:, c]).T.astype(o_ref.dtype)


def attend(q, kv, lo, base, st):
    tc, width = q.shape
    tall = kv.shape[0]
    grp = width // HEAD
    nb = tc // QB
    whole = lambda i, *_: (0, 0)
    rowb = lambda i, *_: (i, 0)
    return pl.pallas_call(
        functools.partial(attn_kernel, grp),
        grid_spec=pltpu.PrefetchScalarGridSpec(
            num_scalar_prefetch=2,
            grid=(nb,),
            in_specs=[
                pl.BlockSpec((QB, width), rowb),
                pl.BlockSpec((tall, 2 * HEAD), whole),
                pl.BlockSpec((1, 1, QB), lambda i, *_: (i, 0, 0)),
            ],
            out_specs=pl.BlockSpec((QB, width), rowb),
            scratch_shapes=[pltpu.VMEM((1, grp * QB), jnp.float32), pltpu.VMEM((1, grp * QB), jnp.float32),
                            pltpu.VMEM((HEAD, grp * QB), jnp.float32), pltpu.VMEM((KB, grp * QB), jnp.float32),
                            pltpu.VMEM((KB, grp * QB), jnp.bfloat16)],
        ),
        out_shape=jax.ShapeDtypeStruct((tc, width), jnp.bfloat16),
        cost_estimate=pl.CostEstimate(flops=tc * width * tall, bytes_accessed=4 * tc * width, transcendentals=0),
        name="attn",
    )(lo, base, q, kv, st)


class Ring:
    def __init__(self, nx, ny, tl):
        self.nx, self.ny, self.tl, self.hf = nx, ny, tl, tl // 2
        t = lax.axis_index('tp')
        self.x = t // 2
        self.c = t % 2
        self.y = lax.axis_index('sp')
        self.right = ((self.x + 1) % nx) * 2 + self.c
        self.left = ((self.x + nx - 1) % nx) * 2 + self.c
        self.partner = self.x * 2 + 1 - self.c
        self.up = (self.y + 1) % ny
        self.down = (self.y + ny - 1) % ny

    def row(self, dx, core, h):
        return pl.multiple_of((((self.x + dx + self.nx) % self.nx) * 2 + core) * self.tl + h * self.hf, self.hf)

    def piece(self, s, i):
        side = (s * (3 - s)) // 2
        dx = side * (2 * i - 1) + 2 * (s // 3)
        flip = (s // 2) * (1 - s // 3)
        return dx, i + flip * (1 - 2 * i)


def rcopy(src, dst, ssem, rsem, dev):
    return pltpu.make_async_remote_copy(src_ref=src, dst_ref=dst, send_sem=ssem, recv_sem=rsem,
                                        device_id=dev, device_id_type=pl.DeviceIdType.MESH)


def barrier(devs):
    b = pltpu.get_barrier_semaphore()
    for d in devs:
        pl.semaphore_signal(b, inc=1, device_id=d, device_id_type=pl.DeviceIdType.MESH)
    pl.semaphore_wait(b, len(devs))


def ids_kernel(nsp, ntp, i_ref, o_ref, ss, rr, s2, r2):
    y, t = lax.axis_index('sp'), lax.axis_index('tp')
    peers = [{'tp': (t + d) % ntp} for d in range(1, ntp)]
    rows = [{'sp': (y + d) % nsp} for d in range(1, nsp)]
    barrier(peers + rows)
    first = [rcopy(i_ref, o_ref.at[y, t], ss.at[d], rr.at[d], peers[d]) for d in range(ntp - 1)]
    for d in first:
        d.start()
    o_ref[y, t] = i_ref[...]
    for d in range(ntp - 1):
        src = (t + ntp - d - 1) % ntp
        rcopy(o_ref.at[y, src], o_ref.at[y, src], ss.at[d], rr.at[d], peers[d]).wait_recv()
    second = [rcopy(o_ref.at[y], o_ref.at[y], s2.at[d], r2.at[d], rows[d]) for d in range(nsp - 1)]
    for d in second:
        d.start()
    for d in range(nsp - 1):
        src = (y + nsp - d - 1) % nsp
        rcopy(o_ref.at[src], o_ref.at[src], s2.at[d], r2.at[d], rows[d]).wait_recv()
    for d in first + second:
        d.wait_send()


def gather_ids(nsp, ntp, seg, pos):
    tl = seg.shape[0]
    own = jnp.zeros((8, tl), jnp.int32).at[0].set(seg).at[1].set(pos)
    dma = pltpu.SemaphoreType.DMA
    return pl.pallas_call(
        functools.partial(ids_kernel, nsp, ntp),
        out_shape=jax.ShapeDtypeStruct((nsp, ntp, 8, tl), jnp.int32),
        in_specs=[VM],
        out_specs=VM,
        scratch_shapes=[dma((ntp - 1,)), dma((ntp - 1,)), dma((nsp - 1,)), dma((nsp - 1,))],
        compiler_params=pltpu.CompilerParams(collective_id=2, has_side_effects=True),
        name="ids",
    )(own)


def in_kernel(l, nx, ny, n_ref, cos_hbm, sin_hbm, wq, wk, wv, wg, wu, q_ref, kv_ref, m_out,
              cos_ref, sin_ref, m_ref, osem, w1, w2, w3, nb, kvs, wsem, rs, rr, ps, pr, ks, kr):
    tl = n_ref.shape[0]
    R = Ring(nx, ny, tl)
    hf, c = R.hf, R.c
    qw = wq.shape[2]
    f = wg.shape[2]
    tc = q_ref.shape[0]
    loads = [
        pltpu.make_async_copy(wq.at[l], w1.at[:, 0:qw], wsem.at[0]),
        pltpu.make_async_copy(wk.at[l], w1.at[:, qw:qw + HEAD], wsem.at[1]),
        pltpu.make_async_copy(wv.at[l], w1.at[:, qw + HEAD:qw + 2 * HEAD], wsem.at[2]),
        pltpu.make_async_copy(cos_hbm, cos_ref, wsem.at[5]),
        pltpu.make_async_copy(sin_hbm, sin_ref, wsem.at[6]),
        pltpu.make_async_copy(wg.at[l], w2, wsem.at[3]),
        pltpu.make_async_copy(wu.at[l], w3, wsem.at[4]),
    ]
    for d in loads:
        d.start()
    side = ({'tp': R.right}, {'tp': R.left})
    mate = {'tp': R.partner}
    rows_ = ({'sp': R.up}, {'sp': R.down})
    barrier([side[0], side[1], mate, rows_[0], rows_[1]])

    def slot(s, i):
        return nb.at[s, pl.ds(pl.multiple_of((2 * i + c) * hf, hf), hf), :]

    def other(s, i):
        return nb.at[s, pl.ds(pl.multiple_of((2 * i + 1 - c) * hf, hf), hf), :]

    def half(h):
        return n_ref.at[pl.ds(h * hf, hf), :]

    def ring(s, i):
        src = slot(1, i) if s == 3 else half(i if s == 1 else 1 - i)
        return rcopy(src, slot(s, i), rs.at[s, i], rr.at[s, i], side[i])

    def ring_in(s, i):
        return rcopy(slot(s, i), slot(s, i), rs.at[s, i], rr.at[s, i], side[i])

    def pass_on(s, i, src):
        return rcopy(src, slot(s, i), ps.at[s, i], pr.at[s, i], mate)

    def pass_in(s, i):
        return rcopy(other(s, i), other(s, i), ps.at[s, i], pr.at[s, i], mate)

    for i in range(2):
        ring(1, i).start()
    for i in range(2):
        pass_on(0, i, half(i)).start()
    for i in range(2):
        ring(2, i).start()
    for i in range(2):
        nb[0, pl.ds(pl.multiple_of((2 * i + c) * hf, hf), hf), :] = n_ref[i * hf:(i + 1) * hf, :]

    def kv_send(s, d, p):
        part = pl.ds((d if p == 0 else 1 - d) * tl, tl)
        k = 2 * d + p
        return rcopy(kvs.at[0, s, part, :], kvs.at[1 + d, s, part, :], ks.at[s, k], kr.at[s, k], rows_[d])

    def kv_fwd(s, d):
        part = pl.ds(d * tl, tl)
        return rcopy(kvs.at[1 + d, s, part, :], kvs.at[3, s, part, :], ks.at[s, 4 + d], kr.at[s, 4 + d], rows_[d])

    def m_copy(s, b, o):
        return pltpu.make_async_copy(m_ref.at[pl.ds(o, hf), :], m_out.at[pl.ds(o, hf), :], osem.at[s, b])

    @pl.loop(0, 4)
    def _(s):
        @pl.when(s > 0)
        def _():
            for i in range(2):
                ring_in(s, i).wait_recv()
                @pl.when(s == 1)
                def _():
                    ring(3, i).start()
                pass_on(s, i, slot(s, i)).start()

        for i in range(2):
            pass_in(s, i).wait_recv()

        @pl.when(s == 0)
        def _():
            for d in loads[:5]:
                d.wait()

        offs = []
        for b in range(4):
            dx, h = R.piece(s, b // 2)
            offs.append(R.row(dx, b % 2, h))
        cs = jnp.concatenate([cos_ref[pl.ds(o, hf), :] for o in offs], axis=0)
        sn = jnp.concatenate([sin_ref[pl.ds(o, hf), :] for o in offs], axis=0)

        def rot(t):
            t = t.astype(jnp.bfloat16).astype(jnp.float32)
            return (t * cs + pltpu.roll(t, HEAD // 2, 1) * sn).astype(jnp.bfloat16)

        kv = mm(nb[s], w1[:, qw:])
        kvs[0, s, :, :HEAD] = rot(kv[:, :HEAD])
        kvs[0, s, :, HEAD:] = kv[:, HEAD:].astype(jnp.bfloat16)
        q = mm(nb[s], w1[:, :qw])
        for p in range(2):
            for d in range(2):
                kv_send(s, d, p).start()
        for j in range(qw // HEAD):
            qh = rot(q[:, j * HEAD:(j + 1) * HEAD])
            for b in range(4):
                q_ref[pl.ds(offs[b], hf), j * HEAD:(j + 1) * HEAD] = qh[b * hf:(b + 1) * hf]

        @pl.when(s == 0)
        def _():
            for d in loads[5:]:
                d.wait()

        @pl.loop(0, f // FT)
        def _(j):
            cols = pl.ds(pl.multiple_of(j * FT, FT), FT)
            g = mm(nb[s], w2[:, cols]).astype(jnp.bfloat16).astype(jnp.float32)
            u = mm(nb[s], w3[:, cols]).astype(jnp.bfloat16).astype(jnp.float32)
            m = (g * jax.nn.sigmoid(g) * u).astype(jnp.bfloat16)
            for b in range(4):
                m_ref[pl.ds(offs[b], hf), cols] = m[b * hf:(b + 1) * hf]

        for d in range(2):
            kv_send(s, d, 0).wait_recv()
            kv_fwd(s, d).start()
        for b in range(4):
            m_copy(s, b, offs[b]).start()

    for i in range(2):
        for s in range(1, 4):
            ring(s, i).wait_send()
        for s in range(4):
            pass_on(s, i, slot(s, i)).wait_send()

    dy = (0, ny - 1, 1, 2)

    def put(src, s):
        base = ((R.y + dy[src]) % ny) * tc
        for b in range(4):
            dx, h = R.piece(s, b // 2)
            kv_ref[pl.ds(pl.multiple_of(base + R.row(dx, b % 2, h), hf), hf), :] = kvs[src, s, b * hf:(b + 1) * hf, :]

    @pl.loop(0, 4)
    def _(s):
        for d in range(2):
            kv_send(s, d, 1).wait_recv()
        for src in range(3):
            put(src, s)

    @pl.loop(0, 4)
    def _(s):
        for d in range(2):
            kv_fwd(s, d).wait_recv()
            kv_fwd(s, d).wait_send()
            for p in range(2):
                kv_send(s, d, p).wait_send()
        for b in range(4):
            m_copy(s, b, b * hf).wait()
        put(3, s)


def stage_in(l, nx, ny, n, cosf, sinf, wq, wk, wv, wg, wu):
    tl, width = n.shape
    tc = cosf.shape[0]
    qw, f = wq.shape[2], wg.shape[2]
    bf = jnp.bfloat16
    dma = pltpu.SemaphoreType.DMA
    flops = 2 * tc * width * (qw + 2 * HEAD + 2 * f)
    return pl.pallas_call(
        functools.partial(in_kernel, l, nx, ny),
        out_shape=(jax.ShapeDtypeStruct((tc, qw), bf),
                   jax.ShapeDtypeStruct((ny * tc, 2 * HEAD), bf),
                   jax.ShapeDtypeStruct((tc, f), bf)),
        in_specs=[VM, ANY, ANY, ANY, ANY, ANY, ANY, ANY],
        out_specs=(VM, VM, ANY),
        scratch_shapes=[
            pltpu.VMEM((tc, HEAD), jnp.float32),
            pltpu.VMEM((tc, HEAD), jnp.float32),
            pltpu.VMEM((tc, f), bf),
            dma((4, 4)),
            pltpu.VMEM((width, qw + 2 * HEAD), bf),
            pltpu.VMEM((width, f), bf),
            pltpu.VMEM((width, f), bf),
            pltpu.VMEM((4, 2 * tl, width), bf),
            pltpu.VMEM((4, 4, 2 * tl, 2 * HEAD), bf),
            dma((7,)), dma((4, 2)), dma((4, 2)), dma((4, 2)), dma((4, 2)), dma((4, 6)), dma((4, 6)),
        ],
        compiler_params=pltpu.CompilerParams(collective_id=0, has_side_effects=True, vmem_limit_bytes=VMEM_LIMIT),
        cost_estimate=pl.CostEstimate(flops=flops, bytes_accessed=2 * width * (qw + 2 * HEAD + 2 * f), transcendentals=0),
        name="gather_in",
    )(n, cosf, sinf, wq, wk, wv, wg, wu)


def out_kernel(l, nx, ny, a_ref, m_ref, h_ref, g_ref, wo, wd, ho_ref, no_ref,
               w1, w2, own, psend, precv, csend, rin, wsem, ps, pr, rs, rr):
    tl, width = h_ref.shape
    R = Ring(nx, ny, tl)
    hf, c = R.hf, R.c
    nt = min(512, width)

    def load(j):
        cols = pl.ds(pl.multiple_of(j * nt, nt), nt)
        return (pltpu.make_async_copy(wo.at[l, :, cols], w1.at[:, cols], wsem.at[j, 0]),
                pltpu.make_async_copy(wd.at[l, :, cols], w2.at[:, cols], wsem.at[j, 1]))

    for j in range(width // nt):
        for d in load(j):
            d.start()
    side = ({'tp': R.right}, {'tp': R.left})
    mate = {'tp': R.partner}
    barrier([side[0], side[1], mate])

    dest = (((2, 0), (2, 1)), ((1, 1), (-1, 0)), ((1, 0), (-1, 1)), ((0, 0), (0, 1)))

    def give(s):
        return rcopy(psend.at[s], precv.at[s], ps.at[s], pr.at[s], mate)

    def send(s, i):
        part = pl.ds(i * hf, hf)
        return rcopy(csend.at[s, part, :], rin.at[s, part, :], rs.at[s, i], rr.at[s, i], side[i])

    def compute(s):
        offs = [R.row(dx, core, h) for core in (1 - c, c) for dx, h in dest[s]]

        @pl.loop(0, width // nt)
        def _(j):
            if s == 0:
                for d in load(j):
                    d.wait()
            cols = pl.ds(pl.multiple_of(j * nt, nt), nt)
            la = jnp.concatenate([a_ref[pl.ds(o, hf), :] for o in offs], axis=0)
            lm = jnp.concatenate([m_ref[pl.ds(o, hf), :] for o in offs], axis=0)
            y = mm(la, w1[:, cols]) + mm(lm, w2[:, cols])
            psend[s, :, cols] = y[:tl].astype(jnp.bfloat16)
            own[:, cols] = y[tl:]

        give(s).start()

    def combine(s):
        give(s).wait_recv()

        @pl.loop(0, width // nt)
        def _(j):
            cols = pl.ds(pl.multiple_of(j * nt, nt), nt)
            t = own[:, cols] + precv[s, :, cols].astype(jnp.float32)
            if s == 2:
                t = t + rin[0, :, cols].astype(jnp.float32)
            csend[s, :, cols] = t.astype(jnp.bfloat16)

        for i in range(2):
            send(s, i).start()

    for s in range(3):
        compute(s)
        if s == 2:
            for i in range(2):
                send(0, i).wait_recv()
        combine(s)
    compute(3)
    give(3).wait_recv()
    for s in (1, 2):
        for i in range(2):
            send(s, i).wait_recv()

    rb = 16

    @pl.loop(0, tl // rb)
    def _(r):
        rows = pl.ds(pl.multiple_of(r * rb, rb), rb)
        top = r // (hf // rb)
        sl = 2 - top
        sr = 1 + top
        inner = pl.multiple_of((r % (hf // rb)) * rb, rb)
        lrow = pl.ds(inner, rb)
        rrow = pl.ds(pl.multiple_of(hf + inner, rb), rb)
        y = own[rows, :] + precv[3, rows, :].astype(jnp.float32)
        y = y + rin[sl, lrow, :].astype(jnp.float32) + rin[sr, rrow, :].astype(jnp.float32)
        hn = (h_ref[rows, :].astype(jnp.float32) + y.astype(jnp.bfloat16).astype(jnp.float32)).astype(jnp.bfloat16)
        ho_ref[rows, :] = hn
        hf32 = hn.astype(jnp.float32)
        inv = lax.rsqrt(jnp.mean(hf32 * hf32, axis=1, keepdims=True) + EPS)
        no_ref[rows, :] = (hf32 * inv * g_ref[...].astype(jnp.float32)).astype(jnp.bfloat16)

    for s in range(4):
        give(s).wait_send()
    for s in range(3):
        for i in range(2):
            send(s, i).wait_send()


def stage_out(l, nx, ny, a, m, h, g, wo, wd):
    tl, width = h.shape
    tc, qw = a.shape
    f = m.shape[1]
    bf = jnp.bfloat16
    dma = pltpu.SemaphoreType.DMA
    return pl.pallas_call(
        functools.partial(out_kernel, l, nx, ny),
        out_shape=(jax.ShapeDtypeStruct((tl, width), bf), jax.ShapeDtypeStruct((tl, width), bf)),
        in_specs=[VM, VM, VM, VM, ANY, ANY],
        out_specs=(VM, VM),
        scratch_shapes=[
            pltpu.VMEM((qw, width), bf),
            pltpu.VMEM((f, width), bf),
            pltpu.VMEM((tl, width), jnp.float32),
            pltpu.VMEM((4, tl, width), bf),
            pltpu.VMEM((4, tl, width), bf),
            pltpu.VMEM((3, tl, width), bf),
            pltpu.VMEM((3, tl, width), bf),
            dma((width // min(512, width), 2)), dma((4,)), dma((4,)), dma((3, 2)), dma((3, 2)),
        ],
        compiler_params=pltpu.CompilerParams(collective_id=1, has_side_effects=True, vmem_limit_bytes=VMEM_LIMIT),
        cost_estimate=pl.CostEstimate(flops=2 * tc * width * (qw + f), bytes_accessed=2 * width * (qw + f), transcendentals=0),
        name="out_scatter",
    )(a, m, h, g, wo, wd)


def solution(mesh):
    nsp = mesh.shape['sp']
    ntp = mesh.shape['tp']
    assert ntp == 8 and nsp == 4
    tok = P(('dp', 'sp', 'tp'))
    tok2 = P(('dp', 'sp', 'tp'), None)
    col = P(None, None, 'tp')
    row = P(None, 'tp', None)

    def body(x, seg, pos, gn, wq, wk, wv, wo, wg, wu, wd):
        tl = x.shape[0]
        tc = tl * ntp
        s = lax.axis_index('sp')
        ids = gather_ids(nsp, ntp, seg, pos)
        seg_all = ids[:, :, 0, :].reshape(nsp * tc)
        mine = lax.dynamic_index_in_dim(ids, s, 0, keepdims=False)
        seg_c = mine[:, 0, :].reshape(tc)
        pos_c = mine[:, 1, :].reshape(tc)
        half = HEAD // 2
        inv = ROPE_THETA ** (-(jnp.arange(half, dtype=jnp.float32) * (2.0 / HEAD)))
        ang = pos_c.astype(jnp.float32)[:, None] * inv[None, :]
        cos, sin = jnp.cos(ang), jnp.sin(ang)
        cosf = jnp.concatenate([cos, cos], axis=1)
        sinf = jnp.concatenate([-sin, sin], axis=1)
        st = jnp.sum((seg_all[:, None] < seg_c[None, :]).astype(jnp.int32), axis=0)
        lo = st[::QB] // KB
        base = (s * tc).astype(jnp.int32).reshape(1)
        st = st.reshape(tc // QB, 1, QB)
        h = x
        n = rms_norm(h, gn[0])
        nl = gn.shape[0]
        for j in range(nl):
            q, kv, m = stage_in(j, ntp // 2, nsp, n, cosf, sinf, wq, wk, wv, wg, wu)
            a = attend(q, kv, lo, base, st)
            g = gn[min(j + 1, nl - 1)].reshape(1, -1)
            h, n = stage_out(j, ntp // 2, nsp, a, m, h, g, wo, wd)
        return h

    return jax.shard_map(body, mesh=mesh,
                         in_specs=(tok2, tok, tok, P(), col, col, col, row, col, col, row),
                         out_specs=tok2, check_vma=False)
```
